32 devices in a mesh: group: 2 (over y), expert: 8 (over z, x), tensor: 2 (over core).
Axes of the slice: x: 2, y: 2, z: 4, core: 2. Of those that a mesh axis runs over, the one named last changes fastest.
Arguments:
- tokens: bfloat16 [16, 256, 1280], P(('group', 'expert'), 'tensor'), parts along dimension 0, may hold values from -6 to 6
- ln_gain: float32 [1280], replicated, may hold values from 0.5 to 1.5
- slot_keys: bfloat16 [1280, 8], P(None, 'expert'), may hold values from -0.3125 to 0.3125
- w_gate: bfloat16 [8, 1280, 1280], P('expert', 'tensor'), may hold values from -0.15625 to 0.15625
- w_up: bfloat16 [8, 1280, 1280], P('expert', 'tensor'), may hold values from -0.15625 to 0.15625
- w_down: bfloat16 [8, 1280, 1280], P('expert', 'tensor'), may hold values from -0.25 to 0.25
Outputs:
- output: bfloat16 [16, 256, 1280], P(('group', 'expert'), 'tensor'), parts along dimension 0
The draws below stay inside these ranges and needn't reach their ends.
There are 2 independent parts, one for each index of `group`. The reference program is written for one: setup_inputs(seed, part) draws one part's arguments, and reference() takes and returns one part's arrays. A program takes and returns all parts, laid end to end along the dimension named above; an argument that names none is the same for every part. Nothing has to cross between parts.
All inputs are finite; a program needn't handle non-finite values.
Results may differ from the reference program's by a relative error of at most 0.0034.
Values may be sent and summed in bfloat16 or wider, within the bound.
A program may use at most 64 MiB of HBM per device.

```python
import jax
import jax.numpy as jnp
from jax import lax

D = 1280
FF = 2560
PATCHES = 256
PER_EXPERT = 2
SLOTS = 8
EXPERTS = 4
IMAGES = 8


def block_scale(rng, extent, cuts, least, high):
    level, own = 1.0, jax.random.fold_in(rng, 6)
    for dim, parts in cuts:
        steps = jnp.exp(jax.random.uniform(jax.random.fold_in(own, dim), (parts,), jnp.float32, least / len(cuts), high / len(cuts)))
        level = level * jnp.repeat(steps, extent[dim] // parts).reshape([-1 if axis == dim else 1 for axis in range(len(extent))])
    return level


def centred(rng, extent, scale, most, cuts=(), held_as=jnp.bfloat16):
    array = jax.random.normal(rng, extent, jnp.float32) * scale
    if len(cuts) > 0:
        array = block_scale(rng, extent, cuts, -0.22, 0.18) * array
    return jnp.clip(array, min=-most, max=most).astype(held_as)


def setup_inputs(seed: int = 0, part: int = 0) -> dict:
    key_of = jax.random.split(jax.random.key(seed), 7)
    own_keys = jax.random.split(jax.random.fold_in(key_of[6], part), 7)
    return {
        "tokens": centred(own_keys[0], (IMAGES, PATCHES, D), 1.0, 6.0, ((0, 8), (1, 2))),
        "ln_gain": jnp.clip(1.0 + 0.1 * jax.random.normal(key_of[1], (D,), jnp.float32), 0.5, 1.5),
        "slot_keys": centred(key_of[2], (D, SLOTS), (D // 4) ** -0.5, 0.3125, ((1, 8),)),
        "w_gate": centred(key_of[3], (2 * EXPERTS, FF // 2, D), D ** -0.5, 0.15625, ((0, 8), (1, 2))),
        "w_up": centred(key_of[4], (2 * EXPERTS, FF // 2, D), D ** -0.5, 0.15625, ((0, 8), (1, 2))),
        "w_down": centred(key_of[5], (2 * EXPERTS, FF // 2, D), (FF // 4) ** -0.5, 0.25, ((0, 8), (1, 2))),
    }


epsilon = 1e-06
soft_cap = 20.0

def layer_norm(tokens, ln_gain):
    widened = tokens.astype(jnp.float32)
    center = widened - lax.optimization_barrier(jnp.mean(widened, axis=-1, keepdims=True))
    variance = lax.optimization_barrier(jnp.mean(center * center, axis=-1, keepdims=True))
    return (center * lax.rsqrt(variance + epsilon) * ln_gain.astype(jnp.float32)).astype(jnp.bfloat16)

def apply_expert(operands):
    rows, gate_w, up_w, down_w = operands
    gate_act = jnp.dot(rows, gate_w.T, preferred_element_type=jnp.float32)
    up_proj = jnp.dot(rows, up_w.T, preferred_element_type=jnp.float32)
    hidden = (jax.nn.silu(gate_act) * up_proj).astype(jnp.bfloat16)
    return jnp.dot(hidden, down_w, preferred_element_type=jnp.float32).astype(jnp.bfloat16)

def reference(tokens, ln_gain, slot_keys, w_gate, w_up, w_down):
    normed = layer_norm(tokens, ln_gain)
    raw_scores = jnp.dot(normed.reshape(-1, D), slot_keys, preferred_element_type=jnp.float32)
    raw_scores = raw_scores.reshape(IMAGES, PATCHES, SLOTS)
    scores = jnp.exp(soft_cap * jnp.tanh(raw_scores / soft_cap))
    scores16 = scores.astype(jnp.bfloat16)
    slot_num = jnp.einsum('ips,ipd->isd', scores16.astype(jnp.float32), normed.astype(jnp.float32))
    column_total = lax.optimization_barrier(jnp.sum(scores, axis=1))
    slot_in = (slot_num / column_total[:, :, None]).astype(jnp.bfloat16)
    by_expert = slot_in.reshape(IMAGES, EXPERTS, PER_EXPERT, D).transpose(1, 2, 0, 3)
    by_expert = by_expert.reshape(EXPERTS, PER_EXPERT * IMAGES, D)
    gate_all = w_gate.reshape(EXPERTS, FF, D)
    up_all = w_up.reshape(EXPERTS, FF, D)
    down_all = w_down.reshape(EXPERTS, FF, D)
    slot_out = lax.map(apply_expert, (by_expert, gate_all, up_all, down_all))
    slot_out = slot_out.reshape(EXPERTS, PER_EXPERT, IMAGES, D).transpose(2, 0, 1, 3).reshape(IMAGES, SLOTS, D)
    combine = (scores / lax.optimization_barrier(jnp.sum(scores, axis=2, keepdims=True))).astype(jnp.bfloat16)
    mixed_rows = jnp.einsum('ips,isd->ipd', combine.astype(jnp.float32), slot_out.astype(jnp.float32))
    return (tokens.astype(jnp.float32) + mixed_rows).astype(jnp.bfloat16)
```

```python
import functools

import jax
import jax.numpy as jnp
from jax import lax
from jax.experimental import pallas as pl
from jax.experimental.pallas import tpu as pltpu
from jax.sharding import PartitionSpec as P

epsilon = 1e-06
soft_cap = 20.0
MESH = pl.DeviceIdType.MESH
f32 = jnp.float32
bf16 = jnp.bfloat16


def repeat(count, body):
    if count <= 16:
        for k in range(count):
            body(k)
    else:
        lax.fori_loop(0, count, lambda k, c: (body(k), c)[1], 0)


def farthest_first(me, n):
    if n & (n - 1):
        return lambda k: lax.rem(me + n - 1 - k, n)

    def peer(k):
        mask, out, bit = n - 1 - k, 0, 1
        while bit < n:
            out = out + ((me // bit + mask // bit) % 2) * bit
            bit *= 2
        return out

    return peer


def layer_kernel(
    n, tokens_hbm, gain_hbm, key_hbm, gate_hbm, up_hbm, down_hbm, out_ref,
    tok, gain_ref, key_ref, gate_w, up_w, down_w, gate_t, up_t, normed, turned, keys, slot_send, arrived, rows,
    out_send, back, load_sem, send_sem, recv_sem, pair_sem,
):
    me = lax.axis_index("expert")
    core = lax.axis_index("tensor")
    half, width = tok.shape
    peer = farthest_first(me, n)

    loads = [
        pltpu.make_async_copy(key_hbm, key_ref, load_sem.at[0]),
        pltpu.make_async_copy(tokens_hbm.at[0], tok, load_sem.at[1]),
        pltpu.make_async_copy(gain_hbm, gain_ref, load_sem.at[2]),
        pltpu.make_async_copy(gate_hbm.at[0], gate_w, load_sem.at[3]),
        pltpu.make_async_copy(up_hbm.at[0], up_w, load_sem.at[4]),
        pltpu.make_async_copy(down_hbm.at[0], down_w, load_sem.at[5]),
    ]
    barrier = pltpu.get_barrier_semaphore()

    def greet(k):
        for c in range(2):
            pl.semaphore_signal(barrier, inc=1, device_id={"expert": peer(k), "tensor": c}, device_id_type=MESH)

    repeat(n - 1, greet)
    pl.semaphore_signal(barrier, inc=1, device_id={"tensor": 1 - core}, device_id_type=MESH)
    for load in loads:
        load.start()
    loads[0].wait()
    pl.semaphore_wait(barrier, 2 * n - 1)

    def send(src, dst, phase, where):
        return pltpu.make_async_remote_copy(
            src_ref=src, dst_ref=dst, send_sem=send_sem.at[phase], recv_sem=recv_sem.at[phase],
            device_id=where, device_id_type=MESH,
        )

    def drain(sems, phase, ref, count):
        whole = ref.at[pl.ds(0, count)]
        pltpu.make_async_copy(whole, whole, sems.at[phase]).wait()

    def pair_copy(which):
        return pltpu.make_async_remote_copy(
            src_ref=normed.at[which], dst_ref=normed.at[which],
            send_sem=pair_sem.at[0], recv_sem=pair_sem.at[1],
            device_id={"tensor": 1 - core}, device_id_type=MESH,
        )

    repeat(n - 1, lambda k: send(key_ref, keys.at[me], 0, {"expert": peer(k), "tensor": 1 - core}).start())
    loads[1].wait()
    widened = tok[...].astype(f32)
    center = widened - jnp.mean(widened, axis=-1, keepdims=True)
    variance = jnp.mean(center * center, axis=-1, keepdims=True)
    loads[2].wait()
    gain = gain_ref[...].reshape(1, width)
    normed[core] = (center * lax.rsqrt(variance + epsilon) * gain).astype(bf16)
    pair_copy(core).start()
    keys[me] = key_ref[...]
    pair_copy(1 - core).wait_recv()
    turned[...] = normed[...].reshape(2 * half, width).T
    drain(recv_sem, 0, keys, n - 1)
    all_keys = keys[...].astype(f32).reshape(n, width).astype(bf16)
    image = normed[...].reshape(2 * half, width)
    raw = lax.dot_general(
        all_keys, turned[...], (((1,), (0,)), ((), ())), preferred_element_type=f32
    )
    scores = jnp.exp(soft_cap * jnp.tanh(raw / soft_cap))
    slot_num = jnp.dot(scores.astype(bf16), image, preferred_element_type=f32)
    slot_in = slot_num / jnp.sum(scores, axis=1, keepdims=True)
    for e in range(n // 2):
        slot_send[e] = slot_in[2 * e:2 * e + 2].astype(bf16)

    def send_slots(k):
        send(slot_send.at[peer(k) // 2], arrived.at[me], 1, {"expert": peer(k), "tensor": 1 - core}).start()

    repeat(n - 1, send_slots)
    arrived[me] = slot_send[me // 2]
    own = jnp.where(core == 0, scores[:, :half], scores[:, half:])
    combine = (own / jnp.sum(own, axis=0, keepdims=True)).astype(bf16)
    loads[3].wait()
    gate_t[...] = gate_w[...].T
    loads[4].wait()
    up_t[...] = up_w[...].T
    loads[5].wait()
    drain(recv_sem, 1, arrived, n - 1)
    for g in range(0, n, 8):
        rows[2 * g:2 * g + 16] = jnp.concatenate(
            [arrived[i].astype(f32) for i in range(g, g + 8)], axis=0
        ).astype(bf16)

    gate_act = jnp.dot(rows[...], gate_t[...], preferred_element_type=f32)
    up_proj = jnp.dot(rows[...], up_t[...], preferred_element_type=f32)
    hidden = (jax.nn.silu(gate_act) * up_proj).astype(bf16)
    part = jnp.dot(hidden, down_w[...], preferred_element_type=f32)
    for i in range(n):
        out_send[i] = part[2 * i:2 * i + 2].astype(bf16)

    mine = 2 * me + core

    def send_out(k):
        for c in range(2):
            send(out_send.at[peer(k)], back.at[mine], 2, {"expert": peer(k), "tensor": c}).start()

    repeat(n - 1, send_out)
    send(out_send.at[me], back.at[mine], 2, {"tensor": 1 - core}).start()
    back[mine] = out_send[me]
    drain(recv_sem, 2, back, 2 * n - 1)
    slot_out = jnp.concatenate(
        [sum(back[4 * e + j].astype(f32) for j in range(4)) for e in range(n // 2)], axis=0
    ).astype(bf16)
    mixed = lax.dot_general(
        combine, slot_out, (((0,), (0,)), ((), ())), preferred_element_type=f32
    )
    out_ref[...] = (tok[...].astype(f32) + mixed).astype(bf16)

    pair_copy(core).wait_send()
    drain(send_sem, 0, keys, n - 1)
    drain(send_sem, 1, arrived, n - 1)
    drain(send_sem, 2, back, 2 * n - 1)


def on_device(tokens, ln_gain, slot_keys, w_gate, w_up, w_down):
    n = lax.axis_size("expert")
    _, half, width = tokens.shape
    units = w_gate.shape[1]
    key_row = slot_keys.reshape(1, width)
    vmem = pl.BlockSpec(memory_space=pltpu.VMEM)
    hbm = pl.BlockSpec(memory_space=pl.ANY)
    out = pl.pallas_call(
        functools.partial(layer_kernel, n),
        out_shape=pltpu.VMEM((half, width), bf16),
        in_specs=[hbm] * 6,
        out_specs=vmem,
        scratch_shapes=[
            pltpu.VMEM((half, width), bf16),
            pltpu.VMEM((width,), f32),
            pltpu.VMEM((1, width), bf16),
            pltpu.VMEM((units, width), bf16),
            pltpu.VMEM((units, width), bf16),
            pltpu.VMEM((units, width), bf16),
            pltpu.VMEM((width, units), bf16),
            pltpu.VMEM((width, units), bf16),
            pltpu.VMEM((2, half, width), bf16),
            pltpu.VMEM((width, 2 * half), bf16),
            pltpu.VMEM((n, 1, width), bf16),
            pltpu.VMEM((n // 2, 2, width), bf16),
            pltpu.VMEM((n, 2, width), bf16),
            pltpu.VMEM((2 * n, width), bf16),
            pltpu.VMEM((n, 2, width), bf16),
            pltpu.VMEM((2 * n, 2, width), bf16),
            pltpu.SemaphoreType.DMA((6,)),
            pltpu.SemaphoreType.DMA((3,)),
            pltpu.SemaphoreType.DMA((3,)),
            pltpu.SemaphoreType.DMA((2,)),
        ],
        compiler_params=pltpu.CompilerParams(collective_id=0, has_side_effects=True),
    )(tokens, ln_gain, key_row, w_gate, w_up, w_down)
    return out[None]


def solution(mesh):
    placed = (
        P(("group", "expert"), "tensor", None),
        P(),
        P(None, "expert"),
        P("expert", "tensor", None),
        P("expert", "tensor", None),
        P("expert", "tensor", None),
    )
    return jax.shard_map(
        on_device,
        mesh=mesh,
        in_specs=placed,
        out_specs=P(("group", "expert"), "tensor", None),
        check_vma=False,
    )
```
